32 devices in a mesh: dp: 8 (over y, x, core), tensor: 4 (over z).
Axes of the slice: x: 2, y: 2, z: 4, core: 2. Of those that a mesh axis runs over, the one named last changes fastest.
Arguments:
- hidden_in: bfloat16 [8192, 2048], P(('dp', 'tensor')), may hold values from -6 to 6
- norm_gains: bfloat16 [4, 2048], P(None, ('dp', 'tensor')), may hold values from 0.5 to 1.5
- q_weight: bfloat16 [2048, 2048], P('dp', 'tensor'), may hold values from -0.125 to 0.125
- k_weight: bfloat16 [2048, 2048], P('dp', 'tensor'), may hold values from -0.125 to 0.125
- v_weight: bfloat16 [2048, 2048], P('dp', 'tensor'), may hold values from -0.125 to 0.125
- o_weight: bfloat16 [2048, 2048], P('tensor', 'dp'), may hold values from -2 to 2
- gate_weight: bfloat16 [16, 2048, 1024], P(None, 'dp', 'tensor'), may hold values from -0.125 to 0.125
- up_weight: bfloat16 [16, 2048, 1024], P(None, 'dp', 'tensor'), may hold values from -0.125 to 0.125
- down_weight: bfloat16 [16, 1024, 2048], P(None, 'tensor', 'dp'), may hold values from -0.1875 to 0.1875
- lengths: int32 [8], P('dp'), may hold values from 1 to 1024, 7424 in all
- routes: int32 [8192, 8], P('dp'), may hold values from 0 to 15, all different within a row; in each aligned block of 1024 rows (0 to 1023, 1024 to 2047, ...) at most 768 rows name the same one
- route_weights: float32 [8192, 8], P('dp'), may hold values from 0.03 to 0.4
- out_grad: bfloat16 [8192, 2048], P(('dp', 'tensor')), may hold values from -6 to 6
Outputs:
- block_out: bfloat16 [8192, 2048], P(('dp', 'tensor'))
- input_grad: float32 [8192, 2048], P(('dp', 'tensor'))
- gains_grad: float32 [4, 2048], P(None, ('dp', 'tensor'))
- q_grad: float32 [2048, 2048], P('dp', 'tensor')
- k_grad: float32 [2048, 2048], P('dp', 'tensor')
- v_grad: float32 [2048, 2048], P('dp', 'tensor')
- o_grad: float32 [2048, 2048], P('tensor', 'dp')
- gate_grad: float32 [16, 2048, 1024], P(None, 'dp', 'tensor')
- up_grad: float32 [16, 2048, 1024], P(None, 'dp', 'tensor')
- down_grad: float32 [16, 1024, 2048], P(None, 'tensor', 'dp')
The draws below stay inside these ranges and needn't reach their ends.
Inputs may be any that keep to these rules, and one draw needn't show every extreme that they name: `routes`: within each slot's 1024 tokens no expert is named by more than 768 tokens, a bound that some block reaches. The lengths sum to 7424 and the longest is exactly 1024.
All inputs are finite; a program needn't handle non-finite values. No bound on the sum of `lengths` on one device may be relied on, other than what follows from the above.
Results may differ from the reference program's by a relative error of at most 0.012.
Values may be sent and summed in bfloat16 or wider, within the bound.
A program may use at most 448 MiB of HBM per device.

```python
import math
import jax
import jax.numpy as jnp
import numpy as np
from jax import lax

D = 2048
HEADS = 16
HEAD_DIM = 128
FF = 1024
EXPERTS = 16
TOP = 8
LEN = 1024
CAP = 768
SLOTS = 8
TOKENS = 8192


def shard_levels(rng, shape, shards, low, high):
    loudness = 1.0
    for axis_at, shards_of in shards:
        heights = jax.random.uniform(jax.random.fold_in(jax.random.fold_in(rng, 6), axis_at), (shards_of,), jnp.float32, low / len(shards), high / len(shards))
        loudness = loudness * jnp.repeat(jnp.exp(heights), shape[axis_at] // shards_of).reshape((-1,) + (1,) * (len(shape) - 1 - axis_at))
    return loudness


def profile(number_of, total, reach, skew):
    loads = [(1 << 20) // math.isqrt(standing ** skew) + 1 for standing in range(2, number_of + 1)]
    spare, counts = total - reach - (number_of - 1), [1] * (number_of - 1)
    while spare > 0:
        movable = [i for i in range(number_of - 1) if counts[i] < reach]
        whole, budget = sum([loads[i] for i in movable]), spare
        for i in movable:
            more = min(reach - counts[i], max(1, budget * loads[i] // whole), spare)
            counts[i] = counts[i] + more
            spare = spare - more
    return np.array([reach] + counts)


def ragged_sizes(own_key, amount, total, limit, lean):
    if amount == 2:
        one = jax.random.randint(own_key, (), max(1, total - limit), min(limit, total - 1) + 1)
        return jnp.stack([one, total - one])
    sizes = jnp.asarray(profile(amount, total, limit, lean), jnp.int32)
    pairs = (amount - 1) // 2
    donor, taker = sizes[1:1 + 2 * pairs:2], sizes[2:2 + 2 * pairs:2]
    margin = jnp.minimum(donor - 1, limit - taker)
    moved = jax.random.randint(jax.random.fold_in(own_key, 1), (pairs,), 0, 1 << 20) % (margin + 1)
    sizes = sizes.at[1:1 + 2 * pairs:2].set(donor - moved).at[2:2 + 2 * pairs:2].set(taker + moved)
    return sizes[jax.random.permutation(jax.random.fold_in(own_key, 2), amount)]


def assign_block(stream_key, own, number, rows, number_of, top, limit, slope):
    order = jax.random.permutation(stream_key, number_of)
    crowded, ordinary = shares(number_of, rows * top, limit, slope, True), shares(number_of, rows * top, limit, slope, False)
    places = jnp.arange(number_of)

    def named(sizes, offset_by):
        used = int((sizes > 0).sum())
        fixed = max(1, used // 4)
        moved = fixed + (places - fixed + offset_by * (used - fixed)) % max(1, number_of - fixed)
        return jnp.zeros((number_of,), jnp.int32).at[order[jnp.where(places < fixed, places, moved)]].set(jnp.asarray(sizes, jnp.int32))

    sizes = jnp.where(number % 4 == 0, named(crowded, number // 4), named(ordinary, number - number // 4 - 1))
    mixed = jax.random.permutation(jax.random.fold_in(own, 3), number_of)
    source_of, sink = mixed[0:number_of // 2 * 2:2], mixed[1:number_of // 2 * 2:2]
    margin = jnp.minimum(sizes[source_of] - 1, limit - sizes[sink]) // 2
    margin = jnp.where((source_of == order[0]) | (sink == order[0]) | (sizes[sink] == 0), 0, jnp.maximum(margin, 0))
    moved = jax.random.randint(jax.random.fold_in(own, 4), (number_of // 2,), 0, 1 << 20) % (margin + 1)
    sizes = sizes.at[source_of].add(-moved).at[sink].add(moved)
    items = jnp.searchsorted(jnp.cumsum(sizes), jnp.arange(rows * top), side="right").astype(jnp.int32)
    table = items.reshape(top, rows).T
    table = table[jax.random.permutation(jax.random.fold_in(own, 1), rows)]
    offset_by = jax.random.randint(jax.random.fold_in(own, 2), (rows, 1), 0, top)
    return jnp.take_along_axis(table, (jnp.arange(top)[None, :] + offset_by) % top, axis=1)


def shares(amount, total, limit, skew, full):
    portions = [(1 << 20) // math.isqrt(grade ** skew) + 1 for grade in range(1, amount + 1)]
    largest = limit if full else min(limit, max(-(-total // amount), total * portions[0] // sum(portions)))
    least = 1 if total - largest >= amount - 1 else 0
    counts, surplus = [largest] + [least] * (amount - 1), total - largest - least * (amount - 1)
    while surplus > 0:
        candidates = [i for i in range(1, amount) if counts[i] < largest] or [i for i in range(1, amount) if counts[i] < limit]
        mass, remaining = sum([portions[i] for i in candidates]), surplus
        for i in candidates:
            extra = min(limit - counts[i], max(1, remaining * portions[i] // mass), surplus)
            counts[i] = counts[i] + extra
            surplus = surplus - extra
    return np.array(counts)


def noise(key, dims, spread, most, cuts=(), held_as=jnp.bfloat16):
    values = jax.random.normal(key, dims, jnp.float32) * spread
    if len(cuts) > 0:
        values = shard_levels(key, dims, cuts, -0.22, 0.18) * values
    return jnp.clip(values, min=-most, max=most).astype(held_as)


def setup_inputs(seed: int = 0) -> dict:
    keys = jax.random.split(jax.random.key(seed), 14)
    hidden_in = noise(keys[0], (TOKENS, D), 1.0, 6.0, ((0, 32),))
    norm_gains = jnp.clip(1.0 + 0.1 * jax.random.normal(keys[1], (4, D), jnp.float32), 0.5, 1.5).astype(jnp.bfloat16)
    q_weight = noise(keys[2], (D, D), D ** -0.5, 0.125, ((0, 8), (1, 4)))
    k_weight = noise(keys[3], (D, D), D ** -0.5, 0.125, ((0, 8), (1, 4)))
    v_weight = noise(keys[4], (D, D), D ** -0.5, 0.125, ((0, 8), (1, 4)))
    o_weight = noise(keys[5], (D, D), (max(D // 256, 1)) ** -0.5, 2.0, ((0, 4), (1, 8)))
    gate_weight = noise(keys[6], (EXPERTS, D, FF), D ** -0.5, 0.125, ((1, 8), (2, 4)))
    up_weight = noise(keys[7], (EXPERTS, D, FF), D ** -0.5, 0.125, ((1, 8), (2, 4)))
    down_weight = noise(keys[8], (EXPERTS, FF, D), FF ** -0.5, 0.1875, ((1, 4), (2, 8)))
    lengths = ragged_sizes(keys[9], SLOTS, SLOTS * LEN * 29 // 32, LEN, 1).astype(jnp.int32)
    routes_keys = jax.random.split(jax.random.fold_in(keys[10], 1), TOKENS // LEN)
    routes_turns = jax.random.permutation(jax.random.fold_in(keys[10], 3), TOKENS // LEN)
    routes = jax.vmap(lambda own, number: assign_block(jax.random.fold_in(keys[10], 2), own, number, LEN, EXPERTS, TOP, CAP, 1))(routes_keys, routes_turns).reshape((TOKENS, TOP))
    route_weights = jnp.clip(jnp.exp(math.log(0.4) - 2.5902672 * jax.random.uniform(keys[11], (TOKENS, TOP), jnp.float32) ** shard_levels(keys[11], (TOKENS, TOP), ((0, 8),), -0.2, 0.2)), 0.03, 0.4)
    out_grad = noise(keys[12], (TOKENS, D), 1.0, 6.0, ((0, 32),))
    return dict(hidden_in=hidden_in, norm_gains=norm_gains, q_weight=q_weight, k_weight=k_weight, v_weight=v_weight, o_weight=o_weight, gate_weight=gate_weight, up_weight=up_weight, down_weight=down_weight, lengths=lengths, routes=routes, route_weights=route_weights, out_grad=out_grad)


norm_eps = 1e-05
highest = lax.Precision.HIGHEST

@jax.custom_vjp
def low(v):
    return lax.optimization_barrier(v.astype(jnp.bfloat16)).astype(jnp.float32)

@jax.custom_vjp
def low_back(v):
    return v

def low_keep(v):
    return (low(v), None)

def low_pass(kept, grad):
    return (grad,)

def back_keep(v):
    return (v, None)

def back_low(kept, grad):
    return (low(grad),)
low.defvjp(low_keep, low_pass)
low_back.defvjp(back_keep, back_low)

def product(left, right):
    return jnp.dot(left, right, precision=highest, preferred_element_type=jnp.float32)

def rms_norm(values, gain):
    return values * lax.rsqrt(lax.optimization_barrier(jnp.mean(values * values, axis=-1, keepdims=True)) + norm_eps) * gain

def rope_tables():
    half_width = HEAD_DIM // 2
    freqs = jnp.exp(-math.log(10000.0) * jnp.arange(half_width, dtype=jnp.float32) / half_width)
    angles = jnp.arange(LEN, dtype=jnp.float32)[:, None] * freqs[None, :]
    return (jnp.cos(angles), jnp.sin(angles))

def rotate(values, cosine_table, sine_table):
    half_width = HEAD_DIM // 2
    front_half = values[..., :half_width]
    back_half = values[..., half_width:]
    cosine_part = cosine_table[:, None, :]
    sine_part = sine_table[:, None, :]
    return jnp.concatenate([front_half * cosine_part - back_half * sine_part, back_half * cosine_part + front_half * sine_part], axis=-1)

def slot_positions(route_rows):
    experts_all = jnp.arange(EXPERTS, dtype=jnp.int32)
    onehot = (route_rows[:, :, None] == experts_all[None, None, :]).astype(jnp.int32)
    chosen = lax.optimization_barrier(jnp.sum(onehot, axis=1))
    before = jnp.cumsum(chosen, axis=0) - chosen
    place = lax.optimization_barrier(jnp.sum(onehot * before[:, None, :], axis=2))
    return route_rows * CAP + place

def slot_layer(params, slot_in):
    gains, q_mat, k_mat, v_mat, o_mat, gate_mat, up_mat, down_mat = params
    stream, route_rows, route_vals, length = slot_in
    positions = jnp.arange(LEN, dtype=jnp.int32)
    valid = (positions < length).astype(jnp.float32)[:, None]
    normed1 = low(rms_norm(stream, gains[0]))
    q_raw = low_back(product(normed1, q_mat))
    k_raw = low_back(product(normed1, k_mat))
    values = low(low_back(product(normed1, v_mat))).reshape(LEN, HEADS, HEAD_DIM)
    cosine_table, sine_table = rope_tables()
    q_rot = low(rotate(rms_norm(q_raw, gains[1]).reshape(LEN, HEADS, HEAD_DIM), cosine_table, sine_table))
    k_rot = low(rotate(rms_norm(k_raw, gains[2]).reshape(LEN, HEADS, HEAD_DIM), cosine_table, sine_table))
    scores = low_back(jnp.einsum('qhd,khd->hqk', q_rot, k_rot, precision=highest) * (1.0 / math.sqrt(HEAD_DIM)))
    allowed = (positions[None, :] <= positions[:, None]) & (positions[None, :] < length)
    scores = jnp.where(allowed[None], scores, -1e+30)
    probs = low(jax.nn.softmax(scores, axis=-1))
    attended = low(low_back(jnp.einsum('hqk,khd->qhd', probs, values, precision=highest).reshape(LEN, D)))
    branch = low_back(product(attended, o_mat))
    mid_stream = stream + valid * branch
    normed2 = low(rms_norm(mid_stream, gains[3]))
    flat = slot_positions(route_rows)
    token_ids = jnp.broadcast_to(positions[:, None], flat.shape)
    source = jnp.full((EXPERTS * CAP,), LEN, jnp.int32).at[flat.reshape(-1)].set(token_ids.reshape(-1))
    padded = jnp.concatenate([normed2, jnp.zeros((1, D), jnp.float32)], axis=0)
    picked = padded[source].reshape(EXPERTS, CAP, D)
    gate_act = low_back(jnp.einsum('ecd,edf->ecf', picked, gate_mat, precision=highest))
    up_act = low_back(jnp.einsum('ecd,edf->ecf', picked, up_mat, precision=highest))
    inner_act = low(jax.nn.silu(gate_act) * up_act)
    expert_out = low_back(jnp.einsum('ecf,efd->ecd', inner_act, down_mat, precision=highest)).reshape(EXPERTS * CAP, D)
    mixed = lax.optimization_barrier(jnp.sum(expert_out[flat] * route_vals[:, :, None], axis=1))
    return mid_stream + valid * mixed

def reference(hidden_in, norm_gains, q_weight, k_weight, v_weight, o_weight, gate_weight, up_weight, down_weight, lengths, routes, route_weights, out_grad):
    params = tuple((weight.astype(jnp.float32) for weight in (norm_gains, q_weight, k_weight, v_weight, o_weight, gate_weight, up_weight, down_weight)))
    stream = hidden_in.astype(jnp.float32).reshape(SLOTS, LEN, D)
    slot_data = (routes.reshape(SLOTS, LEN, TOP), route_weights.reshape(SLOTS, LEN, TOP), lengths)

    def forward(stream_all, params_all):

        def one_slot(inputs):
            return slot_layer(params_all, inputs)
        return lax.map(jax.checkpoint(one_slot), (stream_all,) + slot_data)
    block, pull = jax.vjp(forward, stream, params)
    stream_grad, weight_grads = pull(out_grad.astype(jnp.float32).reshape(SLOTS, LEN, D))
    return (block.reshape(TOKENS, D).astype(jnp.bfloat16), stream_grad.reshape(TOKENS, D), weight_grads[0], weight_grads[1], weight_grads[2], weight_grads[3], weight_grads[4], weight_grads[5], weight_grads[6], weight_grads[7])
```

```python
import functools
import math

import jax
import jax.numpy as jnp
from jax import lax
from jax.experimental import pallas as pl
from jax.experimental.pallas import tpu as pltpu
from jax.sharding import PartitionSpec as P

D = 2048
HEAD_DIM = 128
EXPERTS = 16
LEN = 1024

norm_eps = 1e-05
BF = jnp.bfloat16
F32 = jnp.float32
SCALE = 1.0 / math.sqrt(HEAD_DIM)
NEG = -1e30
VMEM_LIMIT = 60 * 1024 * 1024


def rope_tables():
    half_width = HEAD_DIM // 2
    freqs = jnp.exp(-math.log(10000.0) * jnp.arange(half_width, dtype=F32) / half_width)
    angles = jnp.arange(LEN, dtype=F32)[:, None] * freqs[None, :]
    cosine, sine = jnp.cos(angles), jnp.sin(angles)
    return (
        jnp.concatenate([cosine, cosine], axis=1),
        jnp.concatenate([-sine, sine], axis=1),
    )


def norm_rows(stream):
    scale = lax.rsqrt(jnp.mean(stream * stream, axis=1, keepdims=True) + norm_eps)
    return (stream * scale, scale)


def norm_back(d_normed, unit, scale, gain):
    weighted = d_normed * gain
    return scale * weighted - unit * (scale * jnp.mean(weighted * unit, axis=1, keepdims=True))


def dot_nt(left, right):
    return lax.dot_general(left, right, (((1,), (1,)), ((), ())), preferred_element_type=F32)


def dot_tn(left, right):
    return lax.dot_general(left, right, (((0,), (0,)), ((), ())), preferred_element_type=F32)


def dot(left, right):
    return jnp.dot(left, right, preferred_element_type=F32)


def line_gather(own, count, me):
    rows = own.shape[0]
    rightward = [(i, i + 1) for i in range(count - 1)]
    leftward = [(i + 1, i) for i in range(count - 1)]
    from_left, from_right = [own], [own]
    for step in range(1, count):
        from_left.append(lax.ppermute(from_left[-1], "tensor", rightward[step - 1 :]))
        from_right.append(lax.ppermute(from_right[-1], "tensor", leftward[: count - step]))
    out = jnp.zeros((count * rows,) + own.shape[1:], own.dtype)
    out = lax.dynamic_update_slice_in_dim(out, own, me * rows, 0)
    for step in range(1, count):
        block = jnp.where(me >= step, from_left[step], from_right[count - step])
        out = lax.dynamic_update_slice_in_dim(out, block, lax.rem(me - step + count, count) * rows, 0)
    return out


def line_reduce(partial, count, me):
    rows = partial.shape[0] // count

    def block(index):
        return lax.dynamic_slice_in_dim(partial, lax.rem(index + count, count) * rows, rows, 0)

    left, right = None, None
    for step in range(1, count):
        rightward = [(i, i + 1) for i in range(step)]
        leftward = [(count - 1 - i, count - 2 - i) for i in range(step)]
        to_right, to_left = block(me - step), block(me + step)
        if left is not None:
            to_right = (to_right.astype(F32) + left.astype(F32)).astype(BF)
            to_left = (to_left.astype(F32) + right.astype(F32)).astype(BF)
        left = lax.ppermute(to_right, "tensor", rightward)
        right = lax.ppermute(to_left, "tensor", leftward)
    return block(me).astype(F32) + left.astype(F32) + right.astype(F32)


def small_kernel(axis, count, mode, x_ref, out_ref, held, send_sems, recv_sems):
    me = lax.axis_index(axis)
    barrier = pltpu.get_barrier_semaphore()
    for shift in range(1, count):
        peer = lax.rem(me + shift, count)
        pl.semaphore_signal(barrier, inc=1, device_id={axis: peer}, device_id_type=pl.DeviceIdType.MESH)
    pl.semaphore_wait(barrier, count - 1)
    copies = []
    for shift in range(1, count):
        peer = lax.rem(me + shift, count)
        copies.append(
            pltpu.make_async_remote_copy(
                src_ref=x_ref.at[peer] if mode == "scatter" else x_ref,
                dst_ref=held.at[me],
                send_sem=send_sems.at[shift],
                recv_sem=recv_sems.at[shift],
                device_id={axis: peer},
                device_id_type=pl.DeviceIdType.MESH,
            )
        )
        copies[-1].start()
    held[me] = x_ref[me] if mode == "scatter" else x_ref[...]
    for copy in copies:
        copy.wait()
    if mode == "gather":
        out_ref[...] = held[...]
    else:
        total = held[0]
        for index in range(1, count):
            total = total + held[index]
        out_ref[...] = total


def small_exchange(x, axis, mode, collective_id):
    count = lax.axis_size(axis)
    piece = x.shape[1:] if mode == "scatter" else x.shape
    out_shape = (count,) + piece if mode == "gather" else piece
    return pl.pallas_call(
        functools.partial(small_kernel, axis, count, mode),
        in_specs=[pl.BlockSpec(memory_space=pltpu.VMEM)],
        out_specs=pl.BlockSpec(memory_space=pltpu.VMEM),
        out_shape=jax.ShapeDtypeStruct(out_shape, F32),
        scratch_shapes=[
            pltpu.VMEM((count,) + piece, F32),
            pltpu.SemaphoreType.DMA((count,)),
            pltpu.SemaphoreType.DMA((count,)),
        ],
        compiler_params=pltpu.CompilerParams(collective_id=collective_id, has_side_effects=True),
        name=f"small_{mode}_{collective_id}",
    )(x)


def flip(x, count, bit):
    return lax.ppermute(x, "dp", [(i, i ^ (1 << bit)) for i in range(count)])


def cube_gather(parts, count):
    bits = list(range(1, count.bit_length() - 1))
    orders = (bits, bits[::-1])
    held = []
    for part, order in zip(parts, orders):
        blocks = {0: part}
        for bit in order:
            keys = sorted(blocks)
            got = flip(jnp.stack([blocks[k] for k in keys]), count, bit)
            for n, k in enumerate(keys):
                blocks[k ^ (1 << bit)] = got[n]
        keys = sorted(blocks)
        got = flip(jnp.stack([blocks[k] for k in keys]), count, 0)
        for n, k in enumerate(keys):
            blocks[k ^ 1] = got[n]
        held.append(blocks)
    return held


def cube_pair(keep, away, count):
    return (keep.astype(F32) + flip(away, count, 0).astype(F32)).astype(BF)


def cube_step(parts, count, turn):
    bits = list(range(count.bit_length() - 2))
    out = []
    for blocks, order in zip(parts, (bits, bits[::-1])):
        mask = 1 << order[turn]
        sent = sorted(i for i in blocks if i & mask)
        got = flip(jnp.stack([blocks[i] for i in sent]), count, order[turn] + 1)
        kind = F32 if turn == len(order) - 1 else BF
        out.append(
            {i ^ mask: (blocks[i ^ mask].astype(F32) + got[k].astype(F32)).astype(kind) for k, i in enumerate(sent)}
        )
    return out


def cube_parts(total):
    middle = total.shape[1] // 2
    return [{i: part[i] for i in range(total.shape[0])} for part in (total[:, :middle], total[:, middle:])]


def cube_rest(parts, count, start=0):
    for turn in range(start, count.bit_length() - 2):
        parts = cube_step(parts, count, turn)
    return jnp.concatenate([blocks[0] for blocks in parts], axis=0)


def rotated(values, cosine, sine):
    return values * cosine + pltpu.roll(values, HEAD_DIM // 2, 1) * sine


def rotated_back(values, cosine, sine):
    return values * cosine - pltpu.roll(values, HEAD_DIM // 2, 1) * sine


QBLOCK = 256


def score_mask(row0, extent, length):
    row = lax.broadcasted_iota(jnp.int32, (QBLOCK, extent), 0) + row0
    col = lax.broadcasted_iota(jnp.int32, (QBLOCK, extent), 1)
    return (col <= row) & (col < length)


def attn_fwd_kernel(
    len_ref, q_ref, k_ref, v_ref, qs_ref, ks_ref, gq_ref, gk_ref, cos_ref, sin_ref,
    att_ref, qr_ref, kr_ref, lse_ref,
):
    length = len_ref[0]
    cosine, sine = cos_ref[...], sin_ref[...]
    qr_ref[...] = rotated(q_ref[...] * qs_ref[...] * gq_ref[...], cosine, sine).astype(BF)
    kr_ref[...] = rotated(k_ref[...] * ks_ref[...] * gk_ref[...], cosine, sine).astype(BF)
    for i in range(LEN // QBLOCK):
        extent = (i + 1) * QBLOCK
        rows = slice(i * QBLOCK, extent)
        scores = dot_nt(qr_ref[rows, :], kr_ref[:extent, :]) * SCALE
        scores = jnp.where(score_mask(i * QBLOCK, extent, length), scores, NEG)
        top = jnp.max(scores, axis=1, keepdims=True)
        weights = jnp.exp(scores - top)
        total = jnp.sum(weights, axis=1, keepdims=True)
        probs = (weights * (1.0 / total)).astype(BF)
        att_ref[rows, :] = dot(probs, v_ref[:extent, :]).astype(BF)
        lse_ref[0, rows, :] = top + jnp.log(total)


def column_spec(width=HEAD_DIM):
    return pl.BlockSpec((LEN, width), lambda h, *_: (0, h))


def whole_spec(shape):
    return pl.BlockSpec(shape, lambda h, *_: (0,) * len(shape))


def attention_forward(lengths, q_raw, k_raw, values, q_scale, k_scale, gain_q, gain_k, cosine, sine):
    width = q_raw.shape[1]
    heads = width // HEAD_DIM
    gain_spec = pl.BlockSpec((1, HEAD_DIM), lambda h, *_: (0, h))
    return pl.pallas_call(
        attn_fwd_kernel,
        grid_spec=pltpu.PrefetchScalarGridSpec(
            num_scalar_prefetch=1,
            grid=(heads,),
            in_specs=[column_spec()] * 3
            + [whole_spec((LEN, 1))] * 2
            + [gain_spec] * 2
            + [whole_spec((LEN, HEAD_DIM))] * 2,
            out_specs=[column_spec()] * 3 + [pl.BlockSpec((1, LEN, 1), lambda h, *_: (h, 0, 0))],
        ),
        out_shape=[jax.ShapeDtypeStruct((LEN, width), BF)] * 3
        + [jax.ShapeDtypeStruct((heads, LEN, 1), F32)],
        compiler_params=pltpu.CompilerParams(vmem_limit_bytes=VMEM_LIMIT),
        cost_estimate=pl.CostEstimate(
            flops=4 * LEN * LEN * width, bytes_accessed=16 * LEN * width, transcendentals=heads * LEN * LEN
        ),
        name="attn_fwd",
    )(lengths, q_raw, k_raw, values, q_scale, k_scale, gain_q, gain_k, cosine, sine)


def attn_bwd_kernel(
    len_ref, qr_ref, kr_ref, v_ref, da_ref, lse_ref, q_ref, k_ref, qs_ref, ks_ref, gq_ref, gk_ref, cos_ref, sin_ref,
    dqn_ref, dkn_ref, dv_ref, qsum_ref, ksum_ref, gqg_ref, gkg_ref,
    dk_acc, dv_acc, dq_acc,
):
    length = len_ref[0]
    head = pl.program_id(0)
    dk_acc[...] = jnp.zeros_like(dk_acc)
    dv_acc[...] = jnp.zeros_like(dv_acc)
    for i in range(LEN // QBLOCK):
        extent = (i + 1) * QBLOCK
        rows = slice(i * QBLOCK, extent)
        q_block, k_all, da = qr_ref[rows, :], kr_ref[:extent, :], da_ref[rows, :]
        scores = dot_nt(q_block, k_all) * SCALE
        mask = score_mask(i * QBLOCK, extent, length)
        full = jnp.exp(jnp.where(mask, scores, NEG) - lse_ref[0, rows, :])
        d_probs = dot_nt(da, v_ref[:extent, :])
        inner = jnp.sum(full * d_probs, axis=1, keepdims=True)
        d_scores = (full * (d_probs - inner)).astype(BF)
        dv_acc[:extent, :] += dot_tn(full.astype(BF), da)
        dk_acc[:extent, :] += dot_tn(d_scores, q_block)
        dq_acc[rows, :] = dot(d_scores, k_all)
    cosine, sine = cos_ref[...], sin_ref[...]
    dv_ref[...] = dv_acc[...].astype(BF)
    d_qn = rotated_back(dq_acc[...] * SCALE, cosine, sine)
    d_kn = rotated_back(dk_acc[...] * SCALE, cosine, sine)
    dqn_ref[...] = d_qn
    dkn_ref[...] = d_kn
    q_terms = d_qn * (q_ref[...] * qs_ref[...])
    k_terms = d_kn * (k_ref[...] * ks_ref[...])
    gqg_ref[...] = jnp.sum(q_terms, axis=0, keepdims=True)
    gkg_ref[...] = jnp.sum(k_terms, axis=0, keepdims=True)

    @pl.when(head == 0)
    def _():
        qsum_ref[...] = jnp.zeros_like(qsum_ref)
        ksum_ref[...] = jnp.zeros_like(ksum_ref)

    qsum_ref[...] += jnp.sum(q_terms * gq_ref[...], axis=1, keepdims=True)
    ksum_ref[...] += jnp.sum(k_terms * gk_ref[...], axis=1, keepdims=True)


def attention_backward(
    lengths, q_rot, k_rot, values, d_attended, lse, q_raw, k_raw, q_scale, k_scale, gain_q, gain_k, cosine, sine
):
    width = q_raw.shape[1]
    heads = width // HEAD_DIM
    gain_spec = pl.BlockSpec((1, HEAD_DIM), lambda h, *_: (0, h))
    return pl.pallas_call(
        attn_bwd_kernel,
        grid_spec=pltpu.PrefetchScalarGridSpec(
            num_scalar_prefetch=1,
            grid=(heads,),
            in_specs=[column_spec()] * 4
            + [pl.BlockSpec((1, LEN, 1), lambda h, *_: (h, 0, 0))]
            + [column_spec()] * 2
            + [whole_spec((LEN, 1))] * 2
            + [gain_spec] * 2
            + [whole_spec((LEN, HEAD_DIM))] * 2,
            out_specs=[column_spec()] * 3 + [whole_spec((LEN, 1))] * 2 + [gain_spec] * 2,
            scratch_shapes=[pltpu.VMEM((LEN, HEAD_DIM), F32)] * 3,
        ),
        out_shape=[jax.ShapeDtypeStruct((LEN, width), F32)] * 2
        + [jax.ShapeDtypeStruct((LEN, width), BF)]
        + [jax.ShapeDtypeStruct((LEN, 1), F32)] * 2
        + [jax.ShapeDtypeStruct((1, width), F32)] * 2,
        compiler_params=pltpu.CompilerParams(vmem_limit_bytes=VMEM_LIMIT),
        cost_estimate=pl.CostEstimate(
            flops=10 * LEN * LEN * width, bytes_accessed=28 * LEN * width, transcendentals=heads * LEN * LEN
        ),
        name="attn_bwd",
    )(lengths, q_rot, k_rot, values, d_attended, lse, q_raw, k_raw, q_scale, k_scale, gain_q, gain_k, cosine, sine)


RTILE = 256


def acts_kernel(len_ref, x_ref, cot_ref, routes_ref, rw_ref, wg_ref, wu_ref, wd_ref, dg_ref, du_ref, ic_ref):
    expert = pl.program_id(0)
    length = len_ref[0]
    for r in range(LEN // RTILE):
        rows = slice(r * RTILE, (r + 1) * RTILE)
        gate = dot(x_ref[rows, :], wg_ref[0])
        up = dot(x_ref[rows, :], wu_ref[0])
        d_inner = dot_nt(cot_ref[rows, :], wd_ref[0])
        position = lax.broadcasted_iota(jnp.int32, (RTILE, 8), 0) + r * RTILE
        named = (routes_ref[rows, :] == expert) & (position < length)
        coef = jnp.sum(jnp.where(named, rw_ref[rows, :], 0.0), axis=1, keepdims=True)
        sig = jax.nn.sigmoid(gate)
        silu = gate * sig
        d_inner = d_inner * coef
        dg_ref[rows, :] = (d_inner * up * (sig + silu * (1.0 - sig))).astype(BF)
        du_ref[rows, :] = (d_inner * silu).astype(BF)
        ic_ref[rows, :] = (silu * up * coef).astype(BF)


def expert_acts(lengths, normed2, cot, routes, route_weights, gate_all, up_all, down_all):
    ff = gate_all.shape[2]
    act_spec = pl.BlockSpec((LEN, ff), lambda e, *_: (0, e))
    top = routes.shape[1]
    return pl.pallas_call(
        acts_kernel,
        grid_spec=pltpu.PrefetchScalarGridSpec(
            num_scalar_prefetch=1,
            grid=(EXPERTS,),
            in_specs=[whole_spec((LEN, D))] * 2
            + [whole_spec((LEN, top))] * 2
            + [pl.BlockSpec((1, D, ff), lambda e, *_: (e, 0, 0))] * 2
            + [pl.BlockSpec((1, ff, D), lambda e, *_: (e, 0, 0))],
            out_specs=[act_spec] * 3,
        ),
        out_shape=[jax.ShapeDtypeStruct((LEN, EXPERTS * ff), BF)] * 3,
        compiler_params=pltpu.CompilerParams(vmem_limit_bytes=VMEM_LIMIT),
        cost_estimate=pl.CostEstimate(
            flops=6 * LEN * D * EXPERTS * ff,
            bytes_accessed=6 * EXPERTS * D * ff + 8 * LEN * D,
            transcendentals=LEN * EXPERTS * ff,
        ),
        name="expert_acts",
    )(lengths, normed2, cot, routes, route_weights, gate_all, up_all, down_all)


NTILE = 512


def back_kernel(dg_ref, du_ref, wg_ref, wu_ref, out_ref, acc):
    expert = pl.program_id(0)

    @pl.when(expert == 0)
    def _():
        acc[...] = jnp.zeros_like(acc)

    for c in range(D // NTILE):
        cols = slice(c * NTILE, (c + 1) * NTILE)
        acc[:, cols] += dot_nt(dg_ref[...], wg_ref[0, cols, :]) + dot_nt(du_ref[...], wu_ref[0, cols, :])

    @pl.when(expert == EXPERTS - 1)
    def _():
        out_ref[...] = acc[...].astype(BF)


def expert_back(d_gate, d_up, gate_all, up_all):
    ff = gate_all.shape[2]
    act_spec = pl.BlockSpec((LEN, ff), lambda e: (0, e))
    return pl.pallas_call(
        back_kernel,
        grid=(EXPERTS,),
        in_specs=[act_spec] * 2 + [pl.BlockSpec((1, D, ff), lambda e: (e, 0, 0))] * 2,
        out_specs=whole_spec((LEN, D)),
        out_shape=jax.ShapeDtypeStruct((LEN, D), BF),
        scratch_shapes=[pltpu.VMEM((LEN, D), F32)],
        compiler_params=pltpu.CompilerParams(vmem_limit_bytes=VMEM_LIMIT),
        cost_estimate=pl.CostEstimate(
            flops=4 * LEN * D * EXPERTS * ff, bytes_accessed=4 * EXPERTS * D * ff + 4 * LEN * D, transcendentals=0
        ),
        name="expert_back",
    )(d_gate, d_up, gate_all, up_all)


def mix_kernel(ic_ref, wd_ref, out_ref, acc):
    expert = pl.program_id(0)

    @pl.when(expert == 0)
    def _():
        acc[...] = jnp.zeros_like(acc)

    for c in range(D // NTILE):
        cols = slice(c * NTILE, (c + 1) * NTILE)
        acc[:, cols] += dot(ic_ref[...], wd_ref[0, :, cols])

    @pl.when(expert == EXPERTS - 1)
    def _():
        out_ref[...] = acc[...].astype(BF)


def expert_mix(inner, down_all):
    ff = down_all.shape[1]
    return pl.pallas_call(
        mix_kernel,
        grid=(EXPERTS,),
        in_specs=[pl.BlockSpec((LEN, ff), lambda e: (0, e)), pl.BlockSpec((1, ff, D), lambda e: (e, 0, 0))],
        out_specs=whole_spec((LEN, D)),
        out_shape=jax.ShapeDtypeStruct((LEN, D), BF),
        scratch_shapes=[pltpu.VMEM((LEN, D), F32)],
        compiler_params=pltpu.CompilerParams(vmem_limit_bytes=VMEM_LIMIT),
        cost_estimate=pl.CostEstimate(
            flops=2 * LEN * D * EXPERTS * ff, bytes_accessed=2 * EXPERTS * D * ff + 2 * LEN * D, transcendentals=0
        ),
        name="expert_mix",
    )(inner, down_all)


def col_grad_kernel(xt_ref, act_ref, out_ref):
    for c in range(D // NTILE):
        rows = slice(c * NTILE, (c + 1) * NTILE)
        out_ref[0, rows, :] = dot(xt_ref[rows, :], act_ref[...]).astype(BF)


def expert_col_grad(x_t, acts, name):
    ff = acts.shape[1] // EXPERTS
    return pl.pallas_call(
        col_grad_kernel,
        grid=(EXPERTS,),
        in_specs=[whole_spec((D, LEN)), pl.BlockSpec((LEN, ff), lambda e: (0, e))],
        out_specs=pl.BlockSpec((1, D, ff), lambda e: (e, 0, 0)),
        out_shape=jax.ShapeDtypeStruct((EXPERTS, D, ff), BF),
        compiler_params=pltpu.CompilerParams(vmem_limit_bytes=VMEM_LIMIT),
        cost_estimate=pl.CostEstimate(
            flops=2 * LEN * D * EXPERTS * ff, bytes_accessed=2 * EXPERTS * D * ff + 2 * LEN * D, transcendentals=0
        ),
        name=name,
    )(x_t, acts)


def row_grad_kernel(count, me_ref, cot_ref, act_ref, keep_ref, away_ref):
    block = D // count
    me = me_ref[0]
    for r in range(count):
        cols = pl.ds(pl.multiple_of((me ^ r) * block, block), block)
        out_ref = away_ref if r % 2 else keep_ref
        out_ref[r // 2, 0] = dot_tn(act_ref[...], cot_ref[:, cols]).astype(BF)


def expert_row_grad(acts, cot, me, count):
    ff = acts.shape[1] // EXPERTS
    block = (ff, D // count)
    return pl.pallas_call(
        functools.partial(row_grad_kernel, count),
        grid_spec=pltpu.PrefetchScalarGridSpec(
            num_scalar_prefetch=1,
            grid=(EXPERTS,),
            in_specs=[whole_spec((LEN, D)), pl.BlockSpec((LEN, ff), lambda e, *_: (0, e))],
            out_specs=[pl.BlockSpec((count // 2, 1) + block, lambda e, *_: (0, e, 0, 0))] * 2,
        ),
        out_shape=[jax.ShapeDtypeStruct((count // 2, EXPERTS) + block, BF)] * 2,
        compiler_params=pltpu.CompilerParams(vmem_limit_bytes=VMEM_LIMIT),
        cost_estimate=pl.CostEstimate(
            flops=2 * LEN * D * EXPERTS * ff, bytes_accessed=2 * EXPERTS * D * ff + 2 * LEN * D, transcendentals=0
        ),
        name="expert_down_grad",
    )(me, cot, acts)


def shards(
    hidden_in,
    norm_gains,
    q_weight,
    k_weight,
    v_weight,
    o_weight,
    gate_weight,
    up_weight,
    down_weight,
    lengths,
    routes,
    route_weights,
    out_grad,
):
    count = lax.axis_size("tensor")
    me = lax.axis_index("tensor")
    own_rows = hidden_in.shape[0]
    width = q_weight.shape[1]
    gain_width = norm_gains.shape[1]
    row_start = me * own_rows
    col_start = me * width
    cosine, sine = rope_tables()
    positions = row_start + jnp.arange(own_rows, dtype=jnp.int32)
    valid_own = (positions < lengths[0]).astype(F32)[:, None]

    dp_count = lax.axis_size("dp")
    me_dp = lax.axis_index("dp")

    x_all = line_gather(hidden_in, count, me)
    rows_local = q_weight.shape[0]
    o_side = jnp.concatenate(jnp.split(o_weight, width // rows_local, axis=0), axis=1)
    qk_part = jnp.concatenate([q_weight, k_weight], axis=1)
    vo_part = jnp.concatenate([v_weight, o_side.reshape(rows_local, width)], axis=1)
    qk_blocks, vo_blocks = cube_gather((qk_part, vo_part), dp_count)
    qk_all = jnp.zeros((D, 2 * width), BF)
    v_all = jnp.zeros((D, width), BF)
    o_all = jnp.zeros((width, D), BF)
    for r in range(dp_count):
        at = (me_dp ^ r) * rows_local
        qk_all = lax.dynamic_update_slice_in_dim(qk_all, qk_blocks[r], at, 0)
        v_all = lax.dynamic_update_slice_in_dim(v_all, vo_blocks[r][:, :width], at, 0)
        o_piece = jnp.concatenate(jnp.split(vo_blocks[r][:, width:], width // rows_local, axis=1), axis=0)
        o_all = lax.dynamic_update_slice_in_dim(o_all, o_piece, at, 1)
    gate_all = lax.all_gather(gate_weight, "dp", axis=1, tiled=True)
    up_all = lax.all_gather(up_weight, "dp", axis=1, tiled=True)
    down_all = lax.all_gather(down_weight, "dp", axis=2, tiled=True)
    gain_piece = jnp.pad(norm_gains.astype(F32), ((0, 4), (0, 128 - gain_width)))
    gains = small_exchange(gain_piece, "tensor", "gather", 1).reshape(count * 8, 128)
    gains = small_exchange(gains, "dp", "gather", 2).reshape(dp_count, count, 8, 128)
    gains = gains[:, :, :4, :gain_width].transpose(2, 0, 1, 3).reshape(4, D)
    cot_all = line_gather(lax.optimization_barrier((out_grad, x_all))[0], count, me)

    gain_q = lax.dynamic_slice_in_dim(gains[1], col_start, width)[None, :]
    gain_k = lax.dynamic_slice_in_dim(gains[2], col_start, width)[None, :]
    unit1, _ = norm_rows(x_all.astype(F32))
    normed1 = (unit1 * gains[0]).astype(BF)
    q_raw = dot(normed1, qk_all[:, :width])
    k_raw = dot(normed1, qk_all[:, width:])
    values = dot(normed1, v_all).astype(BF)
    squares = jnp.stack([jnp.sum(q_raw * q_raw, axis=1), jnp.sum(k_raw * k_raw, axis=1)])
    squares = small_exchange(squares.reshape(-1, 128), "tensor", "sum", 3).reshape(2, LEN)
    scales = lax.rsqrt(squares / D + norm_eps)
    q_scale, k_scale = scales[0][:, None], scales[1][:, None]
    attended, q_rot, k_rot, lse = attention_forward(
        lengths, q_raw, k_raw, values, q_scale, k_scale, gain_q, gain_k, cosine, sine
    )
    branch = line_reduce(dot(attended, o_all).astype(BF), count, me)
    x_own = hidden_in.astype(F32)
    mid = x_own + valid_own * branch
    unit2, scale2 = norm_rows(mid)
    normed2_own, cot_all = lax.optimization_barrier(((unit2 * gains[3]).astype(BF), cot_all))
    normed2 = line_gather(normed2_own, count, me)

    d_gate, d_up, inner = expert_acts(lengths, normed2, cot_all, routes, route_weights, gate_all, up_all, down_all)
    back = expert_back(d_gate, d_up, gate_all, up_all)
    back, d_gate, d_up, inner = lax.optimization_barrier((back, d_gate, d_up, inner))
    d_normed2 = line_reduce(back, count, me)
    normed2_t = normed2.T
    gate_part = expert_col_grad(normed2_t, d_gate, "expert_gate_grad")
    up_part = expert_col_grad(normed2_t, d_up, "expert_up_grad")
    down_part = expert_row_grad(inner, cot_all, me_dp.reshape(1), dp_count)
    d_normed2 = lax.optimization_barrier((d_normed2, gate_part, up_part, down_part))[0]
    gate_grad = lax.psum_scatter(gate_part, "dp", scatter_dimension=1, tiled=True).astype(F32)
    up_grad = lax.psum_scatter(up_part, "dp", scatter_dimension=1, tiled=True).astype(F32)
    down_pair = cube_pair(*down_part, dp_count)

    gain2_term = jnp.sum(d_normed2 * unit2, axis=0)
    d_mid = out_grad.astype(F32) + norm_back(d_normed2, unit2, scale2, gains[3])
    d_branch_own, inner = lax.optimization_barrier(((valid_own * d_mid).astype(BF), inner))
    mixed_part = expert_mix(inner, down_all)
    d_branch = line_gather(d_branch_own, count, me)
    d_branch, mixed_part, down_pair = lax.optimization_barrier((d_branch, mixed_part, down_pair))
    down_half = cube_step(cube_parts(down_pair), dp_count, 0)
    mixed = line_reduce(mixed_part, count, me)
    d_attended = dot_nt(d_branch, o_all).astype(BF)
    o_part = dot_tn(attended, d_branch).astype(BF)
    d_qn, d_kn, d_v, q_sum, k_sum, gainq_term, gaink_term = attention_backward(
        lengths, q_rot, k_rot, values, d_attended, lse, q_raw, k_raw, q_scale, k_scale, gain_q, gain_k, cosine, sine
    )
    sums = jnp.stack([q_sum[:, 0], k_sum[:, 0]]).reshape(-1, 128)
    totals = small_exchange(sums, "tensor", "sum", 4).reshape(2, LEN) / D
    d_q = (q_scale * (d_qn * gain_q) - q_raw * (q_scale * q_scale * totals[0][:, None])).astype(BF)
    d_k = (k_scale * (d_kn * gain_k) - k_raw * (k_scale * k_scale * totals[1][:, None])).astype(BF)
    d_qkv = jnp.concatenate([d_q, d_k, d_v], axis=1)
    d_normed1_part = dot_nt(d_qkv[:, : 2 * width], qk_all) + dot_nt(d_v, v_all)
    d_normed1_low, mixed, down_half = lax.optimization_barrier((d_normed1_part.astype(BF), mixed, down_half))
    down_grad = cube_rest(down_half, dp_count, 1)
    d_normed1 = line_reduce(d_normed1_low, count, me)
    qkv_part = dot_tn(normed1, d_qkv).astype(BF)
    gain1_term = jnp.sum(d_normed1_part * unit1, axis=0)

    zero_row = jnp.zeros((D,), F32)
    gain_terms = jnp.stack(
        [
            gain1_term,
            lax.dynamic_update_slice_in_dim(zero_row, gainq_term[0], col_start, 0),
            lax.dynamic_update_slice_in_dim(zero_row, gaink_term[0], col_start, 0),
            gain2_term,
        ],
        axis=0,
    )
    pieces = gain_terms.reshape(4, dp_count, count, gain_width).transpose(2, 1, 0, 3)
    pieces = jnp.pad(pieces, ((0, 0), (0, 0), (0, 4), (0, 128 - gain_width))).reshape(count, dp_count * 8, 128)
    pieces = small_exchange(pieces, "tensor", "scatter", 5).reshape(dp_count, 8, 128)
    gains_grad = small_exchange(pieces, "dp", "scatter", 6)[:4, :gain_width]

    blocks = []
    for r in range(dp_count):
        at = (me_dp ^ r) * rows_local
        o_piece = lax.dynamic_slice_in_dim(o_part, at, rows_local, 1)
        o_piece = jnp.concatenate(jnp.split(o_piece, width // rows_local, axis=0), axis=1)
        blocks.append(jnp.concatenate([lax.dynamic_slice_in_dim(qkv_part, at, rows_local, 0), o_piece], axis=1))
    qkvo_pair = cube_pair(jnp.stack(blocks[0::2]), jnp.stack(blocks[1::2]), dp_count)
    qkvo_grad = cube_rest(cube_parts(qkvo_pair), dp_count)
    q_grad, k_grad, v_grad, o_grad = jnp.split(qkvo_grad, [width, 2 * width, 3 * width], axis=1)
    o_grad = jnp.concatenate(jnp.split(o_grad, width // rows_local, axis=1), axis=0)
    block_out = (mid + mixed).astype(BF)
    unit1_own, scale1_own = norm_rows(x_own)
    input_grad = d_mid + norm_back(d_normed1, unit1_own, scale1_own, gains[0])
    return (
        block_out,
        input_grad,
        gains_grad,
        q_grad,
        k_grad,
        v_grad,
        o_grad,
        gate_grad,
        up_grad,
        down_grad,
    )


def solution(mesh):
    placed = (
        P(("dp", "tensor"), None),
        P(None, ("dp", "tensor")),
        P("dp", "tensor"),
        P("dp", "tensor"),
        P("dp", "tensor"),
        P("tensor", "dp"),
        P(None, "dp", "tensor"),
        P(None, "dp", "tensor"),
        P(None, "tensor", "dp"),
        P("dp"),
        P("dp", None),
        P("dp", None),
        P(("dp", "tensor"), None),
    )
    return jax.shard_map(
        shards,
        mesh=mesh,
        in_specs=placed,
        out_specs=(
            P(("dp", "tensor"), None),
            P(("dp", "tensor"), None),
            P(None, ("dp", "tensor")),
            P("dp", "tensor"),
            P("dp", "tensor"),
            P("dp", "tensor"),
            P("tensor", "dp"),
            P(None, "dp", "tensor"),
            P(None, "dp", "tensor"),
            P(None, "tensor", "dp"),
        ),
        check_vma=False,
    )
```
